32 devices in a mesh: rep: 16 (over z, y, core), tp: 2 (over x).
Axes of the slice: x: 2, y: 2, z: 4, core: 2. Of those that a mesh axis runs over, the one named last changes fastest.
Arguments:
- context: bfloat16 [4096, 3072], P('rep', 'tp'), may hold values from -6 to 6
- residual: bfloat16 [4096, 5120], P(('rep', 'tp')), may hold values from -6 to 6
- cotangent: bfloat16 [4096, 5120], P(('rep', 'tp')), may hold values from -6 to 6
- numer: bfloat16 [16, 3072, 5120], P('rep', 'tp'), may hold values from -0.109375 to 0.109375
- weight: float32 [16], P('rep'), may hold values from 0.5 to 2
- step: int32 [1], replicated, may hold values from 0 to 999999
Outputs:
- output: bfloat16 [4096, 5120], P(('rep', 'tp'))
- grad_context: bfloat16 [4096, 3072], P('rep', 'tp')
- numer_next: bfloat16 [16, 3072, 5120], P('rep', 'tp')
- weight_next: float32 [16], P('rep')
The draws below stay inside these ranges and needn't reach their ends.
All inputs are finite; a program needn't handle non-finite values.
Results may differ from the reference program's by a relative error of at most 0.013.
Values may be sent and summed in bfloat16 or wider, within the bound.
No kernel may reach another device: no remote copies, remote signals or barrier semaphores. Data moves between devices by JAX's collectives and lax.ppermute only.
A program may use at most 192 MiB of HBM per device.

```python
import math
import jax
import jax.numpy as jnp
from jax import lax

D = 5120
TOK = 256
PEER_BITS = 3
HH = 3072
REPS = 16
TOKENS = 4096


def shard_levels(stream_key, shape, shards, low, high):
    def one(axis_at, blocks):
        heights = jax.random.uniform(jax.random.fold_in(jax.random.fold_in(stream_key, 6), axis_at), (blocks,), jnp.float32, low / len(shards), high / len(shards))
        return jnp.repeat(jnp.exp(heights), shape[axis_at] // blocks).reshape((-1,) + (1,) * (len(shape) - axis_at - 1))

    loudness = one(*shards[0])
    for cut in shards[1:]:
        loudness = loudness * one(*cut)
    return loudness


def noise(own_key, extent, deviation, bound, shards=(), held_as=jnp.bfloat16):
    values = deviation * jax.random.normal(own_key, extent, jnp.float32)
    if shards:
        values = values * shard_levels(own_key, extent, shards, -0.22, 0.18)
    return jnp.clip(values, -bound, bound).astype(held_as)


def setup_inputs(seed: int = 0) -> dict:
    splits = jax.random.split(jax.random.key(seed), 7)
    return {
        "context": noise(splits[0], (TOKENS, HH), 1.0, 6.0, ((0, 16), (1, 2))),
        "residual": noise(splits[1], (TOKENS, D), 1.0, 6.0, ((0, 32),)),
        "cotangent": noise(splits[2], (TOKENS, D), 1.0, 6.0, ((0, 32),)),
        "numer": noise(splits[3], (REPS, HH, D), HH ** -0.5, 0.109375, ((0, 16), (1, 2))),
        "weight": jnp.clip(jnp.exp(math.log(2.0) - 1.3862944 * jax.random.uniform(splits[4], (REPS,), jnp.float32) ** shard_levels(splits[4], (REPS,), ((0, 16),), -0.2, 0.2)), 0.5, 2.0),
        "step": jax.random.randint(splits[5], (1,), 0, 1000000).astype(jnp.int32),
    }


LEARN = 0.001


def one_replica(items):
    ctx, resid, cot, numer_r, weight_r, peer_numer = items
    params = (numer_r.astype(jnp.float32) / weight_r).astype(jnp.bfloat16)
    projected = jnp.dot(ctx, params, preferred_element_type=jnp.float32)
    output = (resid.astype(jnp.float32) + projected).astype(jnp.bfloat16)
    grad_ctx = lax.dot_general(cot, params, (((1,), (1,)), ((), ())), preferred_element_type=jnp.float32).astype(jnp.bfloat16)
    grad_params = lax.dot_general(ctx, cot, (((0,), (0,)), ((), ())), preferred_element_type=jnp.float32)
    mixed = 0.5 * (numer_r.astype(jnp.float32) + peer_numer.astype(jnp.float32)) - LEARN * grad_params
    return output, grad_ctx, mixed.astype(jnp.bfloat16)


def reference(context, residual, cotangent, numer, weight, step):
    exponent = jnp.remainder(step[0].astype(jnp.int32), jnp.int32(PEER_BITS + 1)).astype(jnp.int32)
    distance = jnp.left_shift(jnp.int32(1), exponent)
    peer_numer = jnp.roll(numer, distance, axis=0)
    peer_weight = jnp.roll(weight, distance, axis=0)
    ctx = context.reshape(REPS, TOK, HH)
    resid = residual.reshape(REPS, TOK, D)
    cot = cotangent.reshape(REPS, TOK, D)
    output, grad_ctx, numer_next = lax.map(one_replica, (ctx, resid, cot, numer, weight, peer_numer))
    weight_next = 0.5 * (weight + peer_weight)
    return output.reshape(TOKENS, D), grad_ctx.reshape(TOKENS, HH), numer_next, weight_next
```

```python
from functools import partial

import jax
import jax.numpy as jnp
from jax import lax
from jax.experimental import pallas as pl
from jax.experimental.layout import Layout, with_layout_constraint
from jax.experimental.pallas import tpu as pltpu
from jax.sharding import PartitionSpec as P

PEER_BITS = 3


LEARN = 0.001


PIECES = ((23, 1), (0, 8), (8, 12), (20, 2), (22, 1))


def pieces_of(rows):
    if rows % (24 * 16):
        return ((0, rows),)
    unit = rows // 24
    return tuple((start * unit, size * unit) for start, size in PIECES)


def from_behind(block, axis, distance):
    devices = range(lax.axis_size(axis))
    route = [((i - distance) % len(devices), i) for i in devices]
    return lax.ppermute(block, axis, route)


def mix_body(ctx_ref, cot_ref, own_ref, peer_ref, *rest):
    out_ref = rest[-1]
    width = out_ref.shape[1]
    tile = 512 if width % 512 == 0 else width

    @pl.loop(0, width // tile)
    def _(j):
        cols = pl.ds(pl.multiple_of(j * tile, tile), tile)
        grad = jnp.dot(ctx_ref[...], cot_ref[:, cols], preferred_element_type=jnp.float32)
        both = own_ref[:, cols].astype(jnp.float32) + peer_ref[:, cols].astype(jnp.float32)
        out_ref[:, cols] = (0.5 * both - LEARN * grad).astype(out_ref.dtype)


def mix_rows(start, size, ctx_t, cot, own, peer, so_far):
    rows, width = own.shape
    tokens = cot.shape[0]
    block = next(b for b in (128, 64, 32, 16, 8, size) if size % b == 0 and start % b == 0)
    first = start // block
    in_specs = [
        pl.BlockSpec((block, tokens), lambda i: (first + i, 0)),
        pl.BlockSpec((tokens, width), lambda i: (0, 0)),
        pl.BlockSpec((block, width), lambda i: (first + i, 0)),
        pl.BlockSpec((block, width), lambda i: (i, 0)),
    ]
    operands = [ctx_t, cot, own, peer]
    aliases = {}
    if so_far is not None:
        in_specs.append(pl.BlockSpec(memory_space=pl.ANY))
        operands.append(so_far)
        aliases = {4: 0}
    return pl.pallas_call(
        mix_body,
        grid=(size // block,),
        in_specs=in_specs,
        out_specs=pl.BlockSpec((block, width), lambda i: (first + i, 0)),
        out_shape=jax.ShapeDtypeStruct((rows, width), own.dtype),
        input_output_aliases=aliases,
        compiler_params=pltpu.CompilerParams(vmem_limit_bytes=24 * 2**20),
        cost_estimate=pl.CostEstimate(
            flops=2 * size * tokens * width, bytes_accessed=6 * size * width, transcendentals=0
        ),
    )(*operands)


def tail_base(start, size, ctx_t, cot, own):
    grad = jnp.dot(ctx_t[start : start + size], cot, preferred_element_type=jnp.float32)
    return 0.5 * own[start : start + size].astype(jnp.float32) - LEARN * grad


def step_at(bits, context, residual, cotangent, numer, weight):
    distance = 1 << bits
    own_numer = numer[0]
    pieces = pieces_of(own_numer.shape[0])
    peer_weight = from_behind(weight, "rep", distance)
    arrived = []
    source = own_numer
    for start, size in pieces:
        piece = lax.slice_in_dim(source, start, start + size, axis=0)
        source, piece = lax.optimization_barrier((source, piece))
        arrived.append(from_behind(piece, "rep", distance))

    share = lax.axis_size("tp")
    place = lax.axis_index("tp")
    tokens = cotangent.shape[0]
    cot = jnp.zeros((share * tokens, cotangent.shape[1]), cotangent.dtype)
    for away in range(share):
        rows = from_behind(cotangent, "tp", away) if away else cotangent
        cot = lax.dynamic_update_slice(
            cot, rows, (lax.rem(place - away + share, share) * tokens, 0)
        )

    params = (own_numer.astype(jnp.float32) / weight[0]).astype(jnp.bfloat16)
    projected = jnp.dot(context, params, preferred_element_type=jnp.float32)
    total = lax.dynamic_slice_in_dim(projected, place * tokens, tokens, axis=0)
    for away in range(1, share):
        target = lax.rem(place + away, share)
        rows = lax.dynamic_slice_in_dim(projected, target * tokens, tokens, axis=0)
        rows = from_behind(rows.astype(jnp.bfloat16), "tp", away)
        total = total + rows.astype(jnp.float32)
    output = (residual.astype(jnp.float32) + total).astype(jnp.bfloat16)
    output = with_layout_constraint(output, Layout(major_to_minor=(0, 1)))

    grad_ctx = lax.dot_general(
        cot, params, (((1,), (1,)), ((), ())), preferred_element_type=jnp.float32
    ).astype(jnp.bfloat16)

    ctx_t = context.T
    base = tail_base(*pieces[-1], ctx_t, cot, own_numer)
    numer_next = None
    for (start, size), peer in zip(pieces[:-1], arrived[:-1]):
        if numer_next is not None:
            numer_next, peer = lax.optimization_barrier((numer_next, peer))
        numer_next = mix_rows(start, size, ctx_t, cot, own_numer, peer, numer_next)
    numer_next, base, peer_weight = lax.optimization_barrier((numer_next, base, peer_weight))
    weight_next = 0.5 * (weight + peer_weight)
    last = (base + 0.5 * arrived[-1].astype(jnp.float32)).astype(jnp.bfloat16)
    numer_next = lax.dynamic_update_slice(numer_next, last, (pieces[-1][0], 0))
    return output, grad_ctx, numer_next[None], weight_next


def branch(bits, *operands):
    return step_at(bits, *operands)


def on_device(context, residual, cotangent, numer, weight, step):
    exponent = jnp.remainder(step[0], jnp.int32(PEER_BITS + 1))
    branches = [partial(branch, bits) for bits in range(PEER_BITS + 1)]
    return lax.switch(exponent, branches, context, residual, cotangent, numer, weight)


def solution(mesh):
    in_specs = (
        P("rep", "tp"),
        P(("rep", "tp"), None),
        P(("rep", "tp"), None),
        P("rep", "tp", None),
        P("rep"),
        P(),
    )
    out_specs = (P(("rep", "tp"), None), P("rep", "tp"), P("rep", "tp", None), P("rep"))
    return jax.shard_map(
        on_device, mesh=mesh, in_specs=in_specs, out_specs=out_specs, check_vma=False
    )
```

```python
from functools import partial

import jax
import jax.numpy as jnp
from jax import lax
from jax.experimental import pallas as pl
from jax.experimental.layout import Layout, with_layout_constraint
from jax.experimental.pallas import tpu as pltpu
from jax.sharding import PartitionSpec as P

PEER_BITS = 3


LEARN = 0.001


PIECES = ((44, 2), (0, 16), (16, 24), (40, 4), (46, 2))
LONG_PIECES = ((44, 3), (0, 16), (16, 24), (40, 4), (47, 1))


def pieces_of(rows, distance):
    unit = rows // 48
    pieces = PIECES if distance == 1 else LONG_PIECES
    return tuple((start * unit, size * unit) for start, size in pieces)


def from_behind(block, axis, distance):
    devices = range(lax.axis_size(axis))
    route = [((i - distance) % len(devices), i) for i in devices]
    return lax.ppermute(block, axis, route)


def mix_body(tile, ctx_ref, cot_ref, own_ref, peer_ref, *rest):
    out_ref = rest[-1]
    width = out_ref.shape[1]
    first = pl.program_id(1) * width

    @pl.loop(0, width // tile)
    def _(j):
        here = pl.ds(pl.multiple_of(j * tile, tile), tile)
        cols = pl.ds(pl.multiple_of(first + j * tile, tile), tile)
        grad = jnp.dot(ctx_ref[...], cot_ref[:, cols], preferred_element_type=jnp.float32)
        both = own_ref[:, here].astype(jnp.float32) + peer_ref[:, here].astype(jnp.float32)
        out_ref[:, here] = (0.5 * both - LEARN * grad).astype(out_ref.dtype)


def mix_rows(start, size, ctx_t, cot, own, peer, so_far):
    rows, width = own.shape
    tokens = cot.shape[0]
    block = next(b for b in (128, 64, 32, 16, 8, size) if size % b == 0 and start % b == 0)
    first = start // block
    wide = width // 4 if size <= block and width % (4 * 128) == 0 else width
    tile = next(t for t in (640, 512, 256, 128, wide) if wide % t == 0)
    in_specs = [
        pl.BlockSpec((block, tokens), lambda i, j: (first + i, 0)),
        pl.BlockSpec((tokens, width), lambda i, j: (0, 0)),
        pl.BlockSpec((block, wide), lambda i, j: (first + i, j)),
        pl.BlockSpec((block, wide), lambda i, j: (i, j)),
    ]
    operands = [ctx_t, cot, own, peer]
    aliases = {}
    if so_far is not None:
        in_specs.append(pl.BlockSpec(memory_space=pl.ANY))
        operands.append(so_far)
        aliases = {4: 0}
    return pl.pallas_call(
        partial(mix_body, tile),
        grid=(size // block, width // wide),
        in_specs=in_specs,
        out_specs=pl.BlockSpec((block, wide), lambda i, j: (first + i, j)),
        out_shape=jax.ShapeDtypeStruct((rows, width), own.dtype),
        input_output_aliases=aliases,
        compiler_params=pltpu.CompilerParams(vmem_limit_bytes=24 * 2**20),
        cost_estimate=pl.CostEstimate(
            flops=2 * size * tokens * width, bytes_accessed=6 * size * width, transcendentals=0
        ),
    )(*operands)


def tail_base(start, size, ctx_t, cot, own):
    grad = jnp.dot(ctx_t[start : start + size], cot, preferred_element_type=jnp.float32)
    return 0.5 * own[start : start + size].astype(jnp.float32) - LEARN * grad


def step_at(bits, context, residual, cotangent, numer, weight):
    distance = 1 << bits
    own_numer = numer[0]
    pieces = pieces_of(own_numer.shape[0], distance)
    peer_weight = from_behind(weight, "rep", distance)
    arrived = []
    source = own_numer
    for start, size in pieces:
        piece = lax.slice_in_dim(source, start, start + size, axis=0)
        source, piece = lax.optimization_barrier((source, piece))
        arrived.append(from_behind(piece, "rep", distance))

    share = lax.axis_size("tp")
    place = lax.axis_index("tp")
    tokens = cotangent.shape[0]
    cot = jnp.zeros((share * tokens, cotangent.shape[1]), cotangent.dtype)
    for away in range(share):
        rows = from_behind(cotangent, "tp", away) if away else cotangent
        cot = lax.dynamic_update_slice(
            cot, rows, (lax.rem(place - away + share, share) * tokens, 0)
        )

    params = (own_numer.astype(jnp.float32) / weight[0]).astype(jnp.bfloat16)
    projected = jnp.dot(context, params, preferred_element_type=jnp.float32)
    total = lax.dynamic_slice_in_dim(projected, place * tokens, tokens, axis=0)
    for away in range(1, share):
        target = lax.rem(place + away, share)
        rows = lax.dynamic_slice_in_dim(projected, target * tokens, tokens, axis=0)
        rows = from_behind(rows.astype(jnp.bfloat16), "tp", away)
        total = total + rows.astype(jnp.float32)
    output = (residual.astype(jnp.float32) + total).astype(jnp.bfloat16)
    output = with_layout_constraint(output, Layout(major_to_minor=(0, 1)))

    grad_ctx = lax.dot_general(
        cot, params, (((1,), (1,)), ((), ())), preferred_element_type=jnp.float32
    ).astype(jnp.bfloat16)

    ctx_t = context.T
    base = tail_base(*pieces[-1], ctx_t, cot, own_numer)
    numer_next = None
    for (start, size), peer in zip(pieces[:-1], arrived[:-1]):
        if numer_next is not None:
            numer_next, peer = lax.optimization_barrier((numer_next, peer))
        numer_next = mix_rows(start, size, ctx_t, cot, own_numer, peer, numer_next)
    weight_next = 0.5 * (weight + peer_weight)
    numer_next, base, weight_next = lax.optimization_barrier((numer_next, base, weight_next))
    last = (base + 0.5 * arrived[-1].astype(jnp.float32)).astype(jnp.bfloat16)
    numer_next = lax.dynamic_update_slice(numer_next, last, (pieces[-1][0], 0))
    return output, grad_ctx, numer_next[None], weight_next


def branch(bits, *operands):
    return step_at(bits, *operands)


def on_device(context, residual, cotangent, numer, weight, step):
    exponent = jnp.remainder(step[0], jnp.int32(PEER_BITS + 1))
    branches = [partial(branch, bits) for bits in range(PEER_BITS + 1)]
    return lax.switch(exponent, branches, context, residual, cotangent, numer, weight)


def solution(mesh):
    in_specs = (
        P("rep", "tp"),
        P(("rep", "tp"), None),
        P(("rep", "tp"), None),
        P("rep", "tp", None),
        P("rep"),
        P(),
    )
    out_specs = (P(("rep", "tp"), None), P("rep", "tp"), P("rep", "tp", None), P("rep"))
    return jax.shard_map(
        on_device, mesh=mesh, in_specs=in_specs, out_specs=out_specs, check_vma=False
    )
```

```python
from functools import partial

import jax
import jax.numpy as jnp
from jax import lax
from jax.experimental import pallas as pl
from jax.experimental.layout import Layout, with_layout_constraint
from jax.experimental.pallas import tpu as pltpu
from jax.sharding import PartitionSpec as P

PEER_BITS = 3


LEARN = 0.001


PIECES = ((44, 2), (0, 16), (16, 24), (40, 4), (46, 2))


def pieces_of(rows):
    unit = rows // 48
    return tuple((start * unit, size * unit) for start, size in PIECES)


def from_behind(block, axis, distance):
    devices = range(lax.axis_size(axis))
    route = [((i - distance) % len(devices), i) for i in devices]
    return lax.ppermute(block, axis, route)


def mix_body(tile, ctx_ref, cot_ref, own_ref, peer_ref, *rest):
    out_ref = rest[-1]
    width = out_ref.shape[1]
    first = pl.program_id(1) * width

    @pl.loop(0, width // tile)
    def _(j):
        here = pl.ds(pl.multiple_of(j * tile, tile), tile)
        cols = pl.ds(pl.multiple_of(first + j * tile, tile), tile)
        grad = jnp.dot(ctx_ref[...], cot_ref[:, cols], preferred_element_type=jnp.float32)
        both = own_ref[:, here].astype(jnp.float32) + peer_ref[:, here].astype(jnp.float32)
        out_ref[:, here] = (0.5 * both - LEARN * grad).astype(out_ref.dtype)


def mix_rows(start, size, ctx_t, cot, own, peer, so_far):
    rows, width = own.shape
    tokens = cot.shape[0]
    block = next(b for b in (128, 64, 32, 16, 8, size) if size % b == 0 and start % b == 0)
    first = start // block
    wide = width // 4 if size <= block and width % (4 * 128) == 0 else width
    tile = next(t for t in (640, 512, 256, 128, wide) if wide % t == 0)
    in_specs = [
        pl.BlockSpec((block, tokens), lambda i, j: (first + i, 0)),
        pl.BlockSpec((tokens, width), lambda i, j: (0, 0)),
        pl.BlockSpec((block, wide), lambda i, j: (first + i, j)),
        pl.BlockSpec((block, wide), lambda i, j: (i, j)),
    ]
    operands = [ctx_t, cot, own, peer]
    aliases = {}
    if so_far is not None:
        in_specs.append(pl.BlockSpec(memory_space=pl.ANY))
        operands.append(so_far)
        aliases = {4: 0}
    return pl.pallas_call(
        partial(mix_body, tile),
        grid=(size // block, width // wide),
        in_specs=in_specs,
        out_specs=pl.BlockSpec((block, wide), lambda i, j: (first + i, j)),
        out_shape=jax.ShapeDtypeStruct((rows, width), own.dtype),
        input_output_aliases=aliases,
        compiler_params=pltpu.CompilerParams(vmem_limit_bytes=24 * 2**20),
        cost_estimate=pl.CostEstimate(
            flops=2 * size * tokens * width, bytes_accessed=6 * size * width, transcendentals=0
        ),
    )(*operands)


def tail_base(start, size, ctx_t, cot, own):
    grad = jnp.dot(ctx_t[start : start + size], cot, preferred_element_type=jnp.float32)
    return 0.5 * own[start : start + size].astype(jnp.float32) - LEARN * grad


def step_at(bits, context, residual, cotangent, numer, weight, head):
    distance = 1 << bits
    own_numer = numer[0]
    pieces = pieces_of(own_numer.shape[0])
    peer_weight = from_behind(weight, "rep", distance)
    arrived = []
    source = own_numer
    for n, (start, size) in enumerate(pieces):
        piece = lax.slice_in_dim(source, start, start + size, axis=0) if n else head
        source, piece = lax.optimization_barrier((source, piece))
        arrived.append(from_behind(piece, "rep", distance))

    share = lax.axis_size("tp")
    place = lax.axis_index("tp")
    tokens = cotangent.shape[0]
    cot = jnp.zeros((share * tokens, cotangent.shape[1]), cotangent.dtype)
    for away in range(share):
        rows = from_behind(cotangent, "tp", away) if away else cotangent
        cot = lax.dynamic_update_slice(
            cot, rows, (lax.rem(place - away + share, share) * tokens, 0)
        )

    params = (own_numer.astype(jnp.float32) / weight[0]).astype(jnp.bfloat16)
    projected = jnp.dot(context, params, preferred_element_type=jnp.float32)
    total = lax.dynamic_slice_in_dim(projected, place * tokens, tokens, axis=0)
    for away in range(1, share):
        target = lax.rem(place + away, share)
        rows = lax.dynamic_slice_in_dim(projected, target * tokens, tokens, axis=0)
        rows = from_behind(rows.astype(jnp.bfloat16), "tp", away)
        total = total + rows.astype(jnp.float32)
    output = (residual.astype(jnp.float32) + total).astype(jnp.bfloat16)
    output = with_layout_constraint(output, Layout(major_to_minor=(0, 1)))

    grad_ctx = lax.dot_general(
        cot, params, (((1,), (1,)), ((), ())), preferred_element_type=jnp.float32
    ).astype(jnp.bfloat16)

    ctx_t = context.T
    base = tail_base(*pieces[-1], ctx_t, cot, own_numer)
    numer_next = None
    for (start, size), peer in zip(pieces[:-1], arrived[:-1]):
        if numer_next is not None:
            numer_next, peer = lax.optimization_barrier((numer_next, peer))
        numer_next = mix_rows(start, size, ctx_t, cot, own_numer, peer, numer_next)
    weight_next = 0.5 * (weight + peer_weight)
    numer_next, base, weight_next = lax.optimization_barrier((numer_next, base, weight_next))
    last = (base + 0.5 * arrived[-1].astype(jnp.float32)).astype(jnp.bfloat16)
    numer_next = lax.dynamic_update_slice(numer_next, last, (pieces[-1][0], 0))
    return output, grad_ctx, numer_next[None], weight_next


def branch(bits, *operands):
    return step_at(bits, *operands)


def on_device(context, residual, cotangent, numer, weight, step):
    exponent = jnp.remainder(step[0], jnp.int32(PEER_BITS + 1))
    branches = [partial(branch, bits) for bits in range(PEER_BITS + 1)]
    start, size = pieces_of(numer.shape[1])[0]
    head = lax.slice_in_dim(numer[0], start, start + size, axis=0)
    head = lax.optimization_barrier(head)
    return lax.switch(exponent, branches, context, residual, cotangent, numer, weight, head)


def solution(mesh):
    in_specs = (
        P("rep", "tp"),
        P(("rep", "tp"), None),
        P(("rep", "tp"), None),
        P("rep", "tp", None),
        P("rep"),
        P(),
    )
    out_specs = (P(("rep", "tp"), None), P("rep", "tp"), P("rep", "tp", None), P("rep"))
    return jax.shard_map(
        on_device, mesh=mesh, in_specs=in_specs, out_specs=out_specs, check_vma=False
    )
```
